32 devices in a mesh: rows: 2 (over y), cols: 4 (over z), slabs: 2 (over x), trial: 2 (over core).
Axes of the slice: x: 2, y: 2, z: 4, core: 2. Of those that a mesh axis runs over, the one named last changes fastest.
Arguments:
- field_values: float32 [64, 16, 256, 128], P(('trial', 'rows'), 'cols', 'slabs'), parts along dimension 0, may hold values from 0.5 to 2
- conductance: float32 [64, 16, 256, 128], P(('trial', 'rows'), 'cols', 'slabs'), parts along dimension 0, may hold values from 0.03 to 0.15
- source: float32 [64, 16, 256, 128], P(('trial', 'rows'), 'cols', 'slabs'), parts along dimension 0, may hold values from -0.2 to 0.2
Outputs:
- anomaly: float32 [64, 16, 256, 128], P(('trial', 'rows'), 'cols', 'slabs'), parts along dimension 0
- field_values_end: float32 [64, 16, 256, 128], P(('trial', 'rows'), 'cols', 'slabs'), parts along dimension 0
The draws below stay inside these ranges and needn't reach their ends.
There are 2 independent parts, one for each index of `trial`. The reference program is written for one: setup_inputs(seed, part) draws one part's arguments, and reference() takes and returns one part's arrays. A program takes and returns all parts, laid end to end along the dimension named above; each array names one. Nothing has to cross between parts.
All inputs are finite; a program needn't handle non-finite values.
Results may differ from the reference program's by a relative error of at most 0.00002.
Values sent between devices are 32-bit elements; how exact they have to be, the bound alone decides.
A program may use at most 128 MiB of HBM per device.

```python
import jax
import jax.numpy as jnp
from jax import lax

GRID_J = 32
GRID_I = 16
GRID_K = 256
LEVELS = 128
STEPS = 4


def steps_of(own_key, extent, split, least, largest):
    factor_of, own = 1.0, jax.random.fold_in(own_key, 6)
    for dim, shards_of in split:
        draws = jnp.exp(jax.random.uniform(jax.random.fold_in(own, dim), (shards_of,), jnp.float32, least / len(split), largest / len(split)))
        factor_of = factor_of * jnp.repeat(draws, extent[dim] // shards_of).reshape([-1 if axis == dim else 1 for axis in range(len(extent))])
    return factor_of


def setup_inputs(seed: int = 0, part: int = 0) -> dict:
    keys = jax.random.split(jax.random.key(seed), 4)
    part_splits = jax.random.split(jax.random.fold_in(keys[3], part), 4)
    field_values = jnp.clip(0.5 + 1.5 * jax.random.uniform(part_splits[0], (GRID_J, GRID_I, GRID_K, LEVELS), jnp.float32) ** steps_of(part_splits[0], (GRID_J, GRID_I, GRID_K, LEVELS), ((0, 2), (1, 4), (2, 2)), -0.2, 0.2), 0.5, 2.0)
    conductance = jnp.clip(0.03 + 0.120000007 * jax.random.uniform(part_splits[1], (GRID_J, GRID_I, GRID_K, LEVELS), jnp.float32) ** steps_of(part_splits[1], (GRID_J, GRID_I, GRID_K, LEVELS), ((0, 2), (1, 4), (2, 2)), -0.2, 0.2), 0.03, 0.15)
    source = jnp.clip(jax.random.uniform(part_splits[2], (GRID_J, GRID_I, GRID_K, LEVELS), jnp.float32, -0.2, 0.2) * steps_of(part_splits[2], (GRID_J, GRID_I, GRID_K, LEVELS), ((0, 2), (1, 4), (2, 2)), -0.4, 0.0), -0.2, 0.2)
    return dict(field_values=field_values, conductance=conductance, source=source)


def strip_edges(values, dims):
    for dim in dims:
        values = lax.slice_in_dim(values, 1, values.shape[dim] - 1, axis=dim)
    return values

def neighbour(values, dim, start, dims):
    others = [other for other in dims if other != dim]
    values = strip_edges(values, others)
    return lax.slice_in_dim(values, start, start + values.shape[dim] - 2, axis=dim)

def one_step(padded, conductance, source):
    middle = strip_edges(padded, (0, 1, 2))
    lower = [neighbour(padded, dim, 0, (0, 1, 2)) for dim in (0, 1, 2)]
    upper = [neighbour(padded, dim, 2, (0, 1, 2)) for dim in (0, 1, 2)]
    spread = lower[0] + upper[0] + lower[1] + upper[1] + lower[2] + upper[2] - 6.0 * middle
    return middle + conductance * spread + source

def reference(field_values, conductance, source):
    for step in range(STEPS):
        field_values = one_step(jnp.pad(field_values, ((1, 1), (1, 1), (1, 1), (0, 0)), mode='constant'), conductance, source)
    line_mean = lax.optimization_barrier(jnp.mean(field_values, axis=0, keepdims=True))
    centred = field_values - line_mean
    line_variance = lax.optimization_barrier(jnp.mean(centred * centred, axis=0, keepdims=True))
    anomaly = centred * lax.rsqrt(line_variance + 0.0001)
    return (anomaly, field_values)
```

```python
import functools

import jax
import jax.numpy as jnp
from jax import lax
from jax.experimental import pallas as pl
from jax.experimental.pallas import tpu as pltpu
from jax.sharding import PartitionSpec as P

STEPS = 4
CHUNKS = 4
TILE = 8
MESH = pl.DeviceIdType.MESH


def kernel(
    sizes, chunks, field, conductance, source, anomaly, field_end,
    u, cond, src, last, scaled, own, others,
    load_sem, send_sem, recv_sem, ksend_sem, krecv_sem, ssend_sem, srecv_sem, out_sem,
):
    rows, cols, slabs = sizes
    nj, ni, nk, _ = field.shape
    kq = nk // chunks
    row, col, slab = (lax.axis_index(name) for name in ("rows", "cols", "slabs"))
    has = {
        "i-": col > 0, "i+": col < cols - 1,
        "j-": row > 0, "j+": row < rows - 1,
        "k-": slab > 0, "k+": slab < slabs - 1,
    }
    to = {
        "i-": {"cols": jnp.maximum(col - 1, 0)}, "i+": {"cols": jnp.minimum(col + 1, cols - 1)},
        "j-": {"rows": jnp.maximum(row - 1, 0)}, "j+": {"rows": jnp.minimum(row + 1, rows - 1)},
        "k-": {"slabs": jnp.maximum(slab - 1, 0)}, "k+": {"slabs": jnp.minimum(slab + 1, slabs - 1)},
    }
    opposite = {"i-": "i+", "i+": "i-", "j-": "j+", "j+": "j-", "k-": "k+", "k+": "k-"}
    sides = ("i-", "i+", "j-", "j+")
    descending = lax.rem(slab, 2) == 0

    loads = [
        pltpu.make_async_copy(field, u.at[0, pl.ds(1, nj), pl.ds(1, ni), pl.ds(TILE, nk)], load_sem.at[0]),
        pltpu.make_async_copy(conductance, cond, load_sem.at[1]),
        pltpu.make_async_copy(source, src, load_sem.at[2]),
    ]
    loads[0].start()

    barrier = pltpu.get_barrier_semaphore()
    expected = rows - 1
    for off in range(1, rows):
        pl.semaphore_signal(barrier, inc=1, device_id={"rows": lax.rem(row + off, rows)}, device_id_type=MESH)
    for side in ("i-", "i+", "k-", "k+"):
        expected = expected + jnp.where(has[side], 1, 0)

        @pl.when(has[side])
        def _():
            pl.semaphore_signal(barrier, inc=1, device_id=to[side], device_id_type=MESH)

    pl.semaphore_wait(barrier, expected)

    def chunk_of(n):
        return jnp.where(descending, chunks - 1 - n, n)

    def face(side, t, q, first):
        k0 = pl.multiple_of(q * kq, kq)
        inner = pl.ds(pl.multiple_of(TILE + k0, TILE), kq)
        js, is_ = pl.ds(1, nj), pl.ds(1, ni)
        if side[0] == "i":
            here, there = (1, ni + 1) if side == "i-" else (ni, 0)
            dst = u.at[t, js, there, inner]
            start = field.at[:, here - 1, pl.ds(k0, kq)] if first else u.at[t, js, here, inner]
        else:
            here, there = (1, nj + 1) if side == "j-" else (nj, 0)
            dst = u.at[t, there, is_, inner]
            start = field.at[here - 1, :, pl.ds(k0, kq)] if first else u.at[t, here, is_, inner]
        d = sides.index(side)
        return pltpu.make_async_remote_copy(
            src_ref=start, dst_ref=dst, send_sem=send_sem.at[d, t, q], recv_sem=recv_sem.at[d, t, q],
            device_id=to[side], device_id_type=MESH,
        )

    def kface(side, t, first):
        js, is_ = pl.ds(1, nj), pl.ds(1, ni)
        here, there = (TILE, TILE + nk) if side == "k-" else (nk, 0)
        start = field.at[:, :, pl.ds(here - TILE, TILE)] if first else u.at[t, js, is_, pl.ds(here, TILE)]
        d = 0 if side == "k-" else 1
        return pltpu.make_async_remote_copy(
            src_ref=start, dst_ref=u.at[t, js, is_, pl.ds(there, TILE)],
            send_sem=ksend_sem.at[d, t], recv_sem=krecv_sem.at[d, t],
            device_id=to[side], device_id_type=MESH,
        )

    def send_faces(t, q, first):
        for side in sides:
            @pl.when(has[side])
            def _():
                face(side, t, q, first).start()

        @pl.when((q == 0) & has["k-"])
        def _():
            kface("k-", t, first).start()

        @pl.when((q == chunks - 1) & has["k+"])
        def _():
            kface("k+", t, first).start()

    def wait_faces(t, q):
        for side in sides:
            @pl.when(has[opposite[side]])
            def _():
                face(side, t, q, False).wait_recv()

        @pl.when((q == chunks - 1) & has["k+"])
        def _():
            kface("k-", t, False).wait_recv()

        @pl.when((q == 0) & has["k-"])
        def _():
            kface("k+", t, False).wait_recv()

    @pl.loop(0, chunks)
    def _(n):
        send_faces(0, chunk_of(n), True)

    loads[1].start()
    loads[2].start()

    def zero_plane(t, j, i):
        u[t, j, i, pl.ds(TILE, nk)] = jnp.zeros((nk, u.shape[-1]), u.dtype)

    @pl.loop(0, STEPS)
    def _(t):
        for side, i in (("i-", 0), ("i+", ni + 1)):
            @pl.when(jnp.logical_not(has[side]))
            def _():
                @pl.loop(0, nj)
                def _(j):
                    zero_plane(t, j + 1, i)

        for side, j in (("j-", 0), ("j+", nj + 1)):
            @pl.when(jnp.logical_not(has[side]))
            def _():
                for i in range(ni):
                    zero_plane(t, j, i + 1)

        for side, k in (("k-", 0), ("k+", TILE + nk)):
            @pl.when(jnp.logical_not(has[side]))
            def _():
                @pl.loop(0, nj)
                def _(j):
                    for i in range(ni):
                        u[t, j + 1, i + 1, pl.ds(k, TILE)] = jnp.zeros((TILE, u.shape[-1]), u.dtype)

    for load in loads:
        load.wait()

    def stencil(t, j, i, k0):
        inner = pl.ds(pl.multiple_of(TILE + k0, TILE), kq)
        tall = u[t, j + 1, i + 1, pl.ds(k0, kq + 2 * TILE)]
        middle = tall[TILE:TILE + kq]
        spread = u[t, j, i + 1, inner] + u[t, j + 2, i + 1, inner]
        spread = spread + u[t, j + 1, i, inner] + u[t, j + 1, i + 2, inner]
        spread = spread + tall[TILE - 1:TILE - 1 + kq] + tall[TILE + 1:TILE + 1 + kq]
        spread = spread - 6.0 * middle
        own_k = pl.ds(k0, kq)
        return middle + cond[j, i, own_k] * spread + src[j, i, own_k]

    @pl.loop(0, (STEPS - 1) * chunks)
    def _(n):
        t = n // chunks
        q = chunk_of(lax.rem(n, chunks))
        k0 = pl.multiple_of(q * kq, kq)
        wait_faces(t, q)

        @pl.loop(0, nj)
        def _(jj):
            j = lax.rem(jj + nj - 1, nj)
            for i in range(ni):
                u[t + 1, j + 1, i + 1, pl.ds(pl.multiple_of(TILE + k0, TILE), kq)] = stencil(t, j, i, k0)

        send_faces(t + 1, q, False)

    def stats_copy(off, q):
        return pltpu.make_async_remote_copy(
            src_ref=own.at[q], dst_ref=others.at[off - 1, q],
            send_sem=ssend_sem.at[off - 1, q], recv_sem=srecv_sem.at[off - 1, q],
            device_id={"rows": lax.rem(row + off, rows)}, device_id_type=MESH,
        )

    def out_copy(which, q):
        ks = pl.ds(pl.multiple_of(q * kq, kq), kq)
        start, dst = ((last, field_end), (scaled, anomaly))[which]
        return pltpu.make_async_copy(start.at[:, :, ks], dst.at[:, :, ks], out_sem.at[which, q])

    def final_step(n):
        q = chunk_of(n)
        k0 = pl.multiple_of(q * kq, kq)
        ks = pl.ds(k0, kq)
        wait_faces(STEPS - 1, q)

        def step(j, totals):
            sums = []
            for i in range(ni):
                new = stencil(STEPS - 1, j, i, k0)
                last[j, i, ks] = new
                sums.append(totals[i] + new)
            return tuple(sums)

        zero = jnp.zeros((kq, u.shape[-1]), u.dtype)
        totals = lax.fori_loop(0, nj, step, (zero,) * ni)
        for i in range(ni):
            mean = totals[i] / nj
            own[q, 0, i] = mean

            def spread_of(j, total):
                away = last[j, i, ks] - mean
                return total + away * away

            own[q, 1, i] = lax.fori_loop(0, nj, spread_of, zero)
        out_copy(0, q).start()
        for off in range(1, rows):
            stats_copy(off, q).start()

    def finish(n):
        q = chunk_of(n)
        ks = pl.ds(pl.multiple_of(q * kq, kq), kq)
        for off in range(1, rows):
            stats_copy(off, q).wait_recv()
        for i in range(ni):
            means = [own[q, 0, i]] + [others[off - 1, q, 0, i] for off in range(1, rows)]
            spreads = [own[q, 1, i]] + [others[off - 1, q, 1, i] for off in range(1, rows)]
            mean = sum(means[1:], means[0]) / rows
            spread = sum(spreads[1:], spreads[0])
            for other in means:
                spread = spread + nj * ((other - mean) * (other - mean))
            scale = lax.rsqrt(spread / (nj * rows) + 0.0001)

            @pl.loop(0, nj)
            def _(j):
                scaled[j, i, ks] = (last[j, i, ks] - mean) * scale
        out_copy(1, q).start()

    @pl.loop(0, chunks)
    def _(n):
        final_step(n)

        @pl.when(n > 0)
        def _():
            finish(n - 1)

    finish(chunks - 1)

    @pl.loop(0, STEPS * chunks)
    def _(n):
        for side in sides:
            @pl.when(has[side])
            def _():
                face(side, n // chunks, lax.rem(n, chunks), False).wait_send()

    @pl.loop(0, STEPS)
    def _(t):
        for side in ("k-", "k+"):
            @pl.when(has[side])
            def _():
                kface(side, t, False).wait_send()

    @pl.loop(0, chunks)
    def _(q):
        for off in range(1, rows):
            stats_copy(off, q).wait_send()
        out_copy(0, q).wait()
        out_copy(1, q).wait()


def on_device(field_values, conductance, source):
    sizes = tuple(lax.axis_size(name) for name in ("rows", "cols", "slabs"))
    nj, ni, nk, levels = field_values.shape
    chunks = CHUNKS if nk % (CHUNKS * TILE) == 0 else 1
    kq = nk // chunks
    peers = max(sizes[0] - 1, 1)
    whole = jax.ShapeDtypeStruct(field_values.shape, field_values.dtype)
    anywhere = pl.BlockSpec(memory_space=pl.ANY)
    return pl.pallas_call(
        functools.partial(kernel, sizes, chunks),
        out_shape=(whole, whole),
        in_specs=[anywhere] * 3,
        out_specs=(anywhere, anywhere),
        scratch_shapes=[
            pltpu.VMEM((STEPS, nj + 2, ni + 2, nk + 2 * TILE, levels), jnp.float32),
            pltpu.VMEM((nj, ni, nk, levels), jnp.float32),
            pltpu.VMEM((nj, ni, nk, levels), jnp.float32),
            pltpu.VMEM((nj, ni, nk, levels), jnp.float32),
            pltpu.VMEM((nj, ni, nk, levels), jnp.float32),
            pltpu.VMEM((chunks, 2, ni, kq, levels), jnp.float32),
            pltpu.VMEM((peers, chunks, 2, ni, kq, levels), jnp.float32),
            pltpu.SemaphoreType.DMA((3,)),
            pltpu.SemaphoreType.DMA((4, STEPS, chunks)),
            pltpu.SemaphoreType.DMA((4, STEPS, chunks)),
            pltpu.SemaphoreType.DMA((2, STEPS)),
            pltpu.SemaphoreType.DMA((2, STEPS)),
            pltpu.SemaphoreType.DMA((peers, chunks)),
            pltpu.SemaphoreType.DMA((peers, chunks)),
            pltpu.SemaphoreType.DMA((2, chunks)),
        ],
        compiler_params=pltpu.CompilerParams(
            collective_id=0, has_side_effects=True, vmem_limit_bytes=64 * 1024 * 1024 - 65536
        ),
        name="heat_steps",
    )(field_values, conductance, source)


def solution(mesh):
    spec = P(("trial", "rows"), "cols", "slabs", None)
    return jax.shard_map(
        on_device, mesh=mesh, in_specs=(spec,) * 3, out_specs=(spec, spec), check_vma=False
    )
```

```python
import functools

import jax
import jax.numpy as jnp
from jax import lax
from jax.experimental import pallas as pl
from jax.experimental.pallas import tpu as pltpu
from jax.sharding import PartitionSpec as P

STEPS = 4
CHUNKS = 8
TILE = 8
MESH = pl.DeviceIdType.MESH


def kernel(
    sizes, chunks, field, conductance, source, scaled, last,
    u, cond, src, own, others,
    load_sem, send_sem, recv_sem, ksend_sem, krecv_sem, ssend_sem, srecv_sem,
):
    rows, cols, slabs = sizes
    nj, ni, nk, _ = field.shape
    kq = nk // chunks
    row, col, slab = (lax.axis_index(name) for name in ("rows", "cols", "slabs"))
    has = {
        "i-": col > 0, "i+": col < cols - 1,
        "j-": row > 0, "j+": row < rows - 1,
        "k-": slab > 0, "k+": slab < slabs - 1,
    }
    to = {
        "i-": {"cols": jnp.maximum(col - 1, 0)}, "i+": {"cols": jnp.minimum(col + 1, cols - 1)},
        "j-": {"rows": jnp.maximum(row - 1, 0)}, "j+": {"rows": jnp.minimum(row + 1, rows - 1)},
        "k-": {"slabs": jnp.maximum(slab - 1, 0)}, "k+": {"slabs": jnp.minimum(slab + 1, slabs - 1)},
    }
    opposite = {"i-": "i+", "i+": "i-", "j-": "j+", "j+": "j-", "k-": "k+", "k+": "k-"}
    sides = ("i-", "i+", "j-", "j+")
    descending = lax.rem(slab, 2) == 0

    loads = [
        pltpu.make_async_copy(field, u.at[0, pl.ds(1, nj), pl.ds(1, ni), pl.ds(TILE, nk)], load_sem.at[0]),
        pltpu.make_async_copy(conductance, cond, load_sem.at[1]),
        pltpu.make_async_copy(source, src, load_sem.at[2]),
    ]
    loads[0].start()

    barrier = pltpu.get_barrier_semaphore()
    expected = rows - 1
    for off in range(1, rows):
        pl.semaphore_signal(barrier, inc=1, device_id={"rows": lax.rem(row + off, rows)}, device_id_type=MESH)
    for side in ("i-", "i+", "k-", "k+"):
        expected = expected + jnp.where(has[side], 1, 0)

        @pl.when(has[side])
        def _():
            pl.semaphore_signal(barrier, inc=1, device_id=to[side], device_id_type=MESH)

    pl.semaphore_wait(barrier, expected)

    def chunk_of(n):
        return jnp.where(descending, chunks - 1 - n, n)

    def face(side, t, q, first):
        k0 = pl.multiple_of(q * kq, kq)
        inner = pl.ds(pl.multiple_of(TILE + k0, TILE), kq)
        js, is_ = pl.ds(1, nj), pl.ds(1, ni)
        if side[0] == "i":
            here, there = (1, ni + 1) if side == "i-" else (ni, 0)
            dst = u.at[t, js, there, inner]
            start = field.at[:, here - 1, pl.ds(k0, kq)] if first else u.at[t, js, here, inner]
        else:
            here, there = (1, nj + 1) if side == "j-" else (nj, 0)
            dst = u.at[t, there, is_, inner]
            start = field.at[here - 1, :, pl.ds(k0, kq)] if first else u.at[t, here, is_, inner]
        d = sides.index(side)
        return pltpu.make_async_remote_copy(
            src_ref=start, dst_ref=dst, send_sem=send_sem.at[d, t, q], recv_sem=recv_sem.at[d, t, q],
            device_id=to[side], device_id_type=MESH,
        )

    def kface(side, t, first):
        js, is_ = pl.ds(1, nj), pl.ds(1, ni)
        here, there = (TILE, TILE + nk) if side == "k-" else (nk, 0)
        start = field.at[:, :, pl.ds(here - TILE, TILE)] if first else u.at[t, js, is_, pl.ds(here, TILE)]
        d = 0 if side == "k-" else 1
        return pltpu.make_async_remote_copy(
            src_ref=start, dst_ref=u.at[t, js, is_, pl.ds(there, TILE)],
            send_sem=ksend_sem.at[d, t], recv_sem=krecv_sem.at[d, t],
            device_id=to[side], device_id_type=MESH,
        )

    def send_faces(t, q, first):
        for side in sides:
            @pl.when(has[side])
            def _():
                face(side, t, q, first).start()

        @pl.when((q == 0) & has["k-"])
        def _():
            kface("k-", t, first).start()

        @pl.when((q == chunks - 1) & has["k+"])
        def _():
            kface("k+", t, first).start()

    def wait_faces(t, q):
        for side in sides:
            @pl.when(has[opposite[side]])
            def _():
                face(side, t, q, False).wait_recv()

        @pl.when((q == chunks - 1) & has["k+"])
        def _():
            kface("k-", t, False).wait_recv()

        @pl.when((q == 0) & has["k-"])
        def _():
            kface("k+", t, False).wait_recv()

    @pl.loop(0, chunks)
    def _(n):
        send_faces(0, chunk_of(n), True)

    loads[1].start()
    loads[2].start()

    def zero_plane(t, j, i):
        u[t, j, i, pl.ds(TILE, nk)] = jnp.zeros((nk, u.shape[-1]), u.dtype)

    @pl.loop(0, STEPS)
    def _(t):
        for side, i in (("i-", 0), ("i+", ni + 1)):
            @pl.when(jnp.logical_not(has[side]))
            def _():
                @pl.loop(0, nj)
                def _(j):
                    zero_plane(t, j + 1, i)

        for side, j in (("j-", 0), ("j+", nj + 1)):
            @pl.when(jnp.logical_not(has[side]))
            def _():
                for i in range(ni):
                    zero_plane(t, j, i + 1)

        for side, k in (("k-", 0), ("k+", TILE + nk)):
            @pl.when(jnp.logical_not(has[side]))
            def _():
                @pl.loop(0, nj)
                def _(j):
                    for i in range(ni):
                        u[t, j + 1, i + 1, pl.ds(k, TILE)] = jnp.zeros((TILE, u.shape[-1]), u.dtype)

    for load in loads:
        load.wait()

    def stencil(t, j, i, k0):
        inner = pl.ds(pl.multiple_of(TILE + k0, TILE), kq)
        tall = u[t, j + 1, i + 1, pl.ds(k0, kq + 2 * TILE)]
        middle = tall[TILE:TILE + kq]
        spread = u[t, j, i + 1, inner] + u[t, j + 2, i + 1, inner]
        spread = spread + u[t, j + 1, i, inner] + u[t, j + 1, i + 2, inner]
        spread = spread + tall[TILE - 1:TILE - 1 + kq] + tall[TILE + 1:TILE + 1 + kq]
        spread = spread - 6.0 * middle
        own_k = pl.ds(k0, kq)
        return middle + cond[j, i, own_k] * spread + src[j, i, own_k]

    @pl.loop(0, (STEPS - 1) * chunks)
    def _(n):
        t = n // chunks
        q = chunk_of(lax.rem(n, chunks))
        k0 = pl.multiple_of(q * kq, kq)
        wait_faces(t, q)

        @pl.loop(0, nj)
        def _(jj):
            j = lax.rem(jj + nj - 1, nj)
            for i in range(ni):
                u[t + 1, j + 1, i + 1, pl.ds(pl.multiple_of(TILE + k0, TILE), kq)] = stencil(t, j, i, k0)

        send_faces(t + 1, q, False)

    def stats_copy(off, q):
        return pltpu.make_async_remote_copy(
            src_ref=own.at[q], dst_ref=others.at[off - 1, q],
            send_sem=ssend_sem.at[off - 1, q], recv_sem=srecv_sem.at[off - 1, q],
            device_id={"rows": lax.rem(row + off, rows)}, device_id_type=MESH,
        )

    def final_step(n):
        q = chunk_of(n)
        k0 = pl.multiple_of(q * kq, kq)
        ks = pl.ds(k0, kq)
        wait_faces(STEPS - 1, q)

        def step(j, totals):
            sums = []
            for i in range(ni):
                new = stencil(STEPS - 1, j, i, k0)
                last[j, i, ks] = new
                sums.append(totals[i] + new)
            return tuple(sums)

        zero = jnp.zeros((kq, u.shape[-1]), u.dtype)
        totals = lax.fori_loop(0, nj, step, (zero,) * ni)
        for i in range(ni):
            mean = totals[i] / nj
            own[q, 0, i] = mean

            def spread_of(j, total):
                away = last[j, i, ks] - mean
                return total + away * away

            own[q, 1, i] = lax.fori_loop(0, nj, spread_of, zero)
        for off in range(1, rows):
            stats_copy(off, q).start()

    def finish(n):
        q = chunk_of(n)
        ks = pl.ds(pl.multiple_of(q * kq, kq), kq)
        for off in range(1, rows):
            stats_copy(off, q).wait_recv()
        for i in range(ni):
            means = [own[q, 0, i]] + [others[off - 1, q, 0, i] for off in range(1, rows)]
            spreads = [own[q, 1, i]] + [others[off - 1, q, 1, i] for off in range(1, rows)]
            mean = sum(means[1:], means[0]) / rows
            spread = sum(spreads[1:], spreads[0])
            for other in means:
                spread = spread + nj * ((other - mean) * (other - mean))
            scale = lax.rsqrt(spread / (nj * rows) + 0.0001)

            @pl.loop(0, nj)
            def _(j):
                scaled[j, i, ks] = (last[j, i, ks] - mean) * scale

    @pl.loop(0, chunks)
    def _(n):
        final_step(n)

        @pl.when(n > 0)
        def _():
            finish(n - 1)

    finish(chunks - 1)

    @pl.loop(0, STEPS * chunks)
    def _(n):
        for side in sides:
            @pl.when(has[side])
            def _():
                face(side, n // chunks, lax.rem(n, chunks), False).wait_send()

    @pl.loop(0, STEPS)
    def _(t):
        for side in ("k-", "k+"):
            @pl.when(has[side])
            def _():
                kface(side, t, False).wait_send()

    @pl.loop(0, chunks)
    def _(q):
        for off in range(1, rows):
            stats_copy(off, q).wait_send()


def on_device(field_values, conductance, source):
    sizes = tuple(lax.axis_size(name) for name in ("rows", "cols", "slabs"))
    nj, ni, nk, levels = field_values.shape
    chunks = CHUNKS if nk % (CHUNKS * TILE) == 0 else 1
    kq = nk // chunks
    peers = max(sizes[0] - 1, 1)
    whole = pltpu.VMEM(field_values.shape, field_values.dtype)
    near = pl.BlockSpec(memory_space=pltpu.VMEM)
    anywhere = pl.BlockSpec(memory_space=pl.ANY)
    return pl.pallas_call(
        functools.partial(kernel, sizes, chunks),
        out_shape=(whole, whole),
        in_specs=[anywhere] * 3,
        out_specs=(near, near),
        scratch_shapes=[
            pltpu.VMEM((STEPS, nj + 2, ni + 2, nk + 2 * TILE, levels), jnp.float32),
            pltpu.VMEM((nj, ni, nk, levels), jnp.float32),
            pltpu.VMEM((nj, ni, nk, levels), jnp.float32),
            pltpu.VMEM((chunks, 2, ni, kq, levels), jnp.float32),
            pltpu.VMEM((peers, chunks, 2, ni, kq, levels), jnp.float32),
            pltpu.SemaphoreType.DMA((3,)),
            pltpu.SemaphoreType.DMA((4, STEPS, chunks)),
            pltpu.SemaphoreType.DMA((4, STEPS, chunks)),
            pltpu.SemaphoreType.DMA((2, STEPS)),
            pltpu.SemaphoreType.DMA((2, STEPS)),
            pltpu.SemaphoreType.DMA((peers, chunks)),
            pltpu.SemaphoreType.DMA((peers, chunks)),
        ],
        compiler_params=pltpu.CompilerParams(
            collective_id=0, has_side_effects=True, vmem_limit_bytes=52 * 1024 * 1024
        ),
        name="heat_steps",
    )(field_values, conductance, source)


def solution(mesh):
    spec = P(("trial", "rows"), "cols", "slabs", None)
    return jax.shard_map(
        on_device, mesh=mesh, in_specs=(spec,) * 3, out_specs=(spec, spec), check_vma=False
    )
```

```python
import functools

import jax
import jax.numpy as jnp
from jax import lax
from jax.experimental import pallas as pl
from jax.experimental.pallas import tpu as pltpu
from jax.sharding import PartitionSpec as P

STEPS = 4
TILE = 8
PIECES = 4
MESH = pl.DeviceIdType.MESH


def kernel(
    sizes, parts, field, conductance, source, scaled, last,
    u, cond, src, own, others,
    load_sem, send_sem, recv_sem, ksend_sem, krecv_sem, ssend_sem, srecv_sem,
):
    rows, cols, slabs = sizes
    nj, ni, nk, _ = field.shape
    row, col, slab = (lax.axis_index(name) for name in ("rows", "cols", "slabs"))
    has = {
        "i-": col > 0, "i+": col < cols - 1,
        "j-": row > 0, "j+": row < rows - 1,
        "k-": slab > 0, "k+": slab < slabs - 1,
    }
    to = {
        "i-": {"cols": jnp.maximum(col - 1, 0)}, "i+": {"cols": jnp.minimum(col + 1, cols - 1)},
        "j-": {"rows": jnp.maximum(row - 1, 0)}, "j+": {"rows": jnp.minimum(row + 1, rows - 1)},
        "k-": {"slabs": jnp.maximum(slab - 1, 0)}, "k+": {"slabs": jnp.minimum(slab + 1, slabs - 1)},
    }
    opposite = {"i-": "i+", "i+": "i-", "j-": "j+", "j+": "j-", "k-": "k+", "k+": "k-"}
    sides = ("i-", "i+", "j-", "j+")
    descending = lax.rem(slab, 2) == 0

    loads = [
        pltpu.make_async_copy(field, u.at[0, pl.ds(1, nj), pl.ds(1, ni), pl.ds(TILE, nk)], load_sem.at[0]),
        pltpu.make_async_copy(conductance, cond, load_sem.at[1]),
        pltpu.make_async_copy(source, src, load_sem.at[2]),
    ]
    loads[0].start()

    barrier = pltpu.get_barrier_semaphore()
    expected = rows - 1
    for off in range(1, rows):
        pl.semaphore_signal(barrier, inc=1, device_id={"rows": lax.rem(row + off, rows)}, device_id_type=MESH)
    for side in ("i-", "i+", "k-", "k+"):
        expected = expected + jnp.where(has[side], 1, 0)

        @pl.when(has[side])
        def _():
            pl.semaphore_signal(barrier, inc=1, device_id=to[side], device_id_type=MESH)

    pl.semaphore_wait(barrier, expected)

    def start_of(t, n):
        before, size = sum(parts[t][:n]), parts[t][n]
        return pl.multiple_of(jnp.where(descending, nk - before - size, before), TILE)

    def edges_of(t, n):
        first, final = n == 0, n == len(parts[t]) - 1
        low = jnp.where(descending, final, first)
        high = jnp.where(descending, first, final)
        return low, high

    def face(side, t, n, first):
        k0, kq = start_of(t, n), parts[t][n]
        inner = pl.ds(pl.multiple_of(TILE + k0, TILE), kq)
        js, is_ = pl.ds(1, nj), pl.ds(1, ni)
        if side[0] == "i":
            here, there = (1, ni + 1) if side == "i-" else (ni, 0)
            dst = u.at[t, js, there, inner]
            start = field.at[:, here - 1, pl.ds(k0, kq)] if first else u.at[t, js, here, inner]
        else:
            here, there = (1, nj + 1) if side == "j-" else (nj, 0)
            dst = u.at[t, there, is_, inner]
            start = field.at[here - 1, :, pl.ds(k0, kq)] if first else u.at[t, here, is_, inner]
        d = sides.index(side)
        return pltpu.make_async_remote_copy(
            src_ref=start, dst_ref=dst, send_sem=send_sem.at[d, t, n], recv_sem=recv_sem.at[d, t, n],
            device_id=to[side], device_id_type=MESH,
        )

    def kface(side, t, first):
        js, is_ = pl.ds(1, nj), pl.ds(1, ni)
        here, there = (TILE, TILE + nk) if side == "k-" else (nk, 0)
        start = field.at[:, :, pl.ds(here - TILE, TILE)] if first else u.at[t, js, is_, pl.ds(here, TILE)]
        d = 0 if side == "k-" else 1
        return pltpu.make_async_remote_copy(
            src_ref=start, dst_ref=u.at[t, js, is_, pl.ds(there, TILE)],
            send_sem=ksend_sem.at[d, t], recv_sem=krecv_sem.at[d, t],
            device_id=to[side], device_id_type=MESH,
        )

    def send_faces(t, n, first):
        low, high = edges_of(t, n)
        for side in sides:
            @pl.when(has[side])
            def _():
                face(side, t, n, first).start()

        @pl.when(low & has["k-"])
        def _():
            kface("k-", t, first).start()

        @pl.when(high & has["k+"])
        def _():
            kface("k+", t, first).start()

    def wait_faces(t, n):
        low, high = edges_of(t, n)
        for side in sides:
            @pl.when(has[opposite[side]])
            def _():
                face(side, t, n, False).wait_recv()

        @pl.when(high & has["k+"])
        def _():
            kface("k-", t, False).wait_recv()

        @pl.when(low & has["k-"])
        def _():
            kface("k+", t, False).wait_recv()

    for n in range(len(parts[0])):
        send_faces(0, n, True)

    loads[1].start()
    loads[2].start()

    def zero_plane(t, j, i):
        u[t, j, i, pl.ds(TILE, nk)] = jnp.zeros((nk, u.shape[-1]), u.dtype)

    @pl.loop(0, STEPS)
    def _(t):
        for side, i in (("i-", 0), ("i+", ni + 1)):
            @pl.when(jnp.logical_not(has[side]))
            def _():
                @pl.loop(0, nj)
                def _(j):
                    zero_plane(t, j + 1, i)

        for side, j in (("j-", 0), ("j+", nj + 1)):
            @pl.when(jnp.logical_not(has[side]))
            def _():
                for i in range(ni):
                    zero_plane(t, j, i + 1)

        for side, k in (("k-", 0), ("k+", TILE + nk)):
            @pl.when(jnp.logical_not(has[side]))
            def _():
                @pl.loop(0, nj)
                def _(j):
                    for i in range(ni):
                        u[t, j + 1, i + 1, pl.ds(k, TILE)] = jnp.zeros((TILE, u.shape[-1]), u.dtype)

    for load in loads:
        load.wait()

    def stencil(t, j, i, k0, kq):
        inner = pl.ds(pl.multiple_of(TILE + k0, TILE), kq)
        tall = u[t, j + 1, i + 1, pl.ds(k0, kq + 2 * TILE)]
        middle = tall[TILE:TILE + kq]
        spread = u[t, j, i + 1, inner] + u[t, j + 2, i + 1, inner]
        spread = spread + u[t, j + 1, i, inner] + u[t, j + 1, i + 2, inner]
        spread = spread + tall[TILE - 1:TILE - 1 + kq] + tall[TILE + 1:TILE + 1 + kq]
        spread = spread - 6.0 * middle
        own_k = pl.ds(k0, kq)
        return middle + cond[j, i, own_k] * spread + src[j, i, own_k]

    def middle_step(t, n):
        k0, kq = start_of(t, n), parts[t][n]
        wait_faces(t, n)

        @pl.loop(0, nj)
        def _(jj):
            j = lax.rem(jj + nj - 1, nj)
            for i in range(ni):
                u[t + 1, j + 1, i + 1, pl.ds(pl.multiple_of(TILE + k0, TILE), kq)] = stencil(t, j, i, k0, kq)

        low, done = sum(parts[t][:n]), sum(parts[t][:n + 1])
        for m in range(len(parts[t + 1])):
            if low <= sum(parts[t + 1][:m]) < done:
                send_faces(t + 1, m, False)

    for t in range(STEPS - 1):
        for n in range(len(parts[t])):
            middle_step(t, n)

    final = parts[STEPS - 1]

    def span_of(n):
        return pl.ds(start_of(STEPS - 1, n), final[n])

    def stats_copy(off, n):
        return pltpu.make_async_remote_copy(
            src_ref=own.at[:, :, span_of(n)], dst_ref=others.at[off - 1, :, :, span_of(n)],
            send_sem=ssend_sem.at[off - 1, n], recv_sem=srecv_sem.at[off - 1, n],
            device_id={"rows": lax.rem(row + off, rows)}, device_id_type=MESH,
        )

    def final_step(n):
        k0, kq, ks = start_of(STEPS - 1, n), final[n], span_of(n)
        wait_faces(STEPS - 1, n)
        zero = jnp.zeros((kq, u.shape[-1]), u.dtype)
        for i in range(ni):
            def step(j, total):
                new = stencil(STEPS - 1, j, i, k0, kq)
                last[j, i, ks] = new
                return total + new

            mean = lax.fori_loop(0, nj, step, zero, unroll=2) / nj
            own[0, i, ks] = mean

            def spread_of(j, total):
                away = last[j, i, ks] - mean
                return total + away * away

            own[1, i, ks] = lax.fori_loop(0, nj, spread_of, zero, unroll=2)
        for off in range(1, rows):
            stats_copy(off, n).start()

    def finish(n):
        ks = span_of(n)
        for off in range(1, rows):
            stats_copy(off, n).wait_recv()
        for i in range(ni):
            means = [own[0, i, ks]] + [others[off - 1, 0, i, ks] for off in range(1, rows)]
            spreads = [own[1, i, ks]] + [others[off - 1, 1, i, ks] for off in range(1, rows)]
            mean = sum(means[1:], means[0]) / rows
            spread = sum(spreads[1:], spreads[0])
            for other in means:
                spread = spread + nj * ((other - mean) * (other - mean))
            scale = lax.rsqrt(spread / (nj * rows) + 0.0001)

            @pl.loop(0, nj)
            def _(j):
                scaled[j, i, ks] = (last[j, i, ks] - mean) * scale

    for n in range(len(final)):
        final_step(n)
        if n > 0:
            finish(n - 1)
    finish(len(final) - 1)

    for t in range(STEPS):
        for side in sides:
            @pl.when(has[side])
            def _():
                for n in range(len(parts[t])):
                    face(side, t, n, False).wait_send()

        for side in ("k-", "k+"):
            @pl.when(has[side])
            def _():
                kface(side, t, False).wait_send()

    for n in range(len(final)):
        for off in range(1, rows):
            stats_copy(off, n).wait_send()


def write_out(near_anomaly, near_field, anomaly, field_end, sems):
    copies = []
    for which, (start, dst) in enumerate(((near_field, field_end), (near_anomaly, anomaly))):
        pieces = sems.shape[1]
        depth = start.shape[0] // pieces
        for piece in range(pieces):
            js = pl.ds(piece * depth, depth)
            copies.append(pltpu.make_async_copy(start.at[js], dst.at[js], sems.at[which, piece]))
    for copy in copies:
        copy.start()
    for copy in copies:
        copy.wait()


def parts_of(nk):
    half = nk // 2 if nk % (2 * TILE) == 0 else nk
    coarse = (half,) * (nk // half)
    small = half * 3 // 8 // TILE * TILE
    fine = coarse[:-1] + ((half - small, small) if small else (half,))
    return (coarse,) * (STEPS - 1) + (fine,)


def on_device(field_values, conductance, source):
    sizes = tuple(lax.axis_size(name) for name in ("rows", "cols", "slabs"))
    nj, ni, nk, levels = field_values.shape
    parts = parts_of(nk)
    most = max(len(of) for of in parts)
    peers = max(sizes[0] - 1, 1)
    whole = pltpu.VMEM(field_values.shape, field_values.dtype)
    near = pl.BlockSpec(memory_space=pltpu.VMEM)
    anywhere = pl.BlockSpec(memory_space=pl.ANY)
    results = pl.pallas_call(
        functools.partial(kernel, sizes, parts),
        out_shape=(whole, whole),
        in_specs=[anywhere] * 3,
        out_specs=(near, near),
        scratch_shapes=[
            pltpu.VMEM((STEPS, nj + 2, ni + 2, nk + 2 * TILE, levels), jnp.float32),
            pltpu.VMEM((nj, ni, nk, levels), jnp.float32),
            pltpu.VMEM((nj, ni, nk, levels), jnp.float32),
            pltpu.VMEM((2, ni, nk, levels), jnp.float32),
            pltpu.VMEM((peers, 2, ni, nk, levels), jnp.float32),
            pltpu.SemaphoreType.DMA((3,)),
            pltpu.SemaphoreType.DMA((4, STEPS, most)),
            pltpu.SemaphoreType.DMA((4, STEPS, most)),
            pltpu.SemaphoreType.DMA((2, STEPS)),
            pltpu.SemaphoreType.DMA((2, STEPS)),
            pltpu.SemaphoreType.DMA((peers, most)),
            pltpu.SemaphoreType.DMA((peers, most)),
        ],
        compiler_params=pltpu.CompilerParams(
            collective_id=0, has_side_effects=True, vmem_limit_bytes=52 * 1024 * 1024
        ),
        name="heat_steps",
    )(field_values, conductance, source)
    there = jax.ShapeDtypeStruct(field_values.shape, field_values.dtype)
    pieces = PIECES if nj % PIECES == 0 else 1
    return pl.pallas_call(
        write_out,
        out_shape=(there, there),
        in_specs=[near] * 2,
        out_specs=(anywhere, anywhere),
        scratch_shapes=[pltpu.SemaphoreType.DMA((2, pieces))],
        compiler_params=pltpu.CompilerParams(vmem_limit_bytes=1024 * 1024),
        name="write_out",
    )(*results)


def solution(mesh):
    spec = P(("trial", "rows"), "cols", "slabs", None)
    return jax.shard_map(
        on_device, mesh=mesh, in_specs=(spec,) * 3, out_specs=(spec, spec), check_vma=False
    )
```
